32 devices in a mesh: row: 16 (over z, y, core), col: 2 (over x).
Axes of the slice: x: 2, y: 2, z: 4, core: 2. Of those that a mesh axis runs over, the one named last changes fastest.
Arguments:
- start: float32 [32768, 128], P(('row', 'col')), may hold values from -18 to 18
- couplings: bfloat16 [128, 5, 256, 256], P(('row', 'col')), may hold values from -0.15625 to 0.15625
- tile_cols: int32 [128, 5], P(('row', 'col')), may hold values from 0 to 19
- stiffness: float32 [32768], P(('row', 'col')), may hold values from 1.5 to 4
- masses: float32 [32768], P(('row', 'col')), may hold values from 0.8 to 2.5, as said below
- bounds: float32 [2], replicated, may hold values from 1.8 to 6.5, as said below
Outputs:
- basis: float32 [32768, 128], P(('row', 'col'))
- ritz: float32 [128, 128], replicated
The draws below stay inside these ranges and needn't reach their ends.
Inputs may be any that keep to these rules, and one draw needn't show every extreme that they name: Positive masses. bounds[0] < bounds[1].
All inputs are finite; a program needn't handle non-finite values.
Results may differ from the reference program's by a relative error of at most 0.0014.
Values may be sent and summed in bfloat16 or wider, within the bound.
No kernel may reach another device: no remote copies, remote signals or barrier semaphores. Data moves between devices by JAX's collectives and lax.ppermute only.
A program may use at most 64 MiB of HBM per device.

```python
import math
import jax
import jax.numpy as jnp
from jax import lax

K = 128
TILE = 256
TILES_ROW = 5
DEGREE = 8
ROWS_DEV = 1024
NODES = 32768
N_ROW = 16
N_COL = 2


def draw_start(key, part):
    progress = jnp.arange(NODES, dtype=jnp.float32) / NODES
    noise = jnp.clip(jax.random.normal(jax.random.fold_in(key, 19), (NODES, K), jnp.float32), -6.0, 6.0)
    scale = 1.0 + 2.0 * progress
    return noise * scale[:, None]


def draw_masses(key, part):
    progress = jnp.arange(NODES, dtype=jnp.float32) / NODES
    baseline = 1.5 + 0.0 * progress
    roughness = jnp.exp(jax.random.uniform(jax.random.fold_in(key, 11), (NODES,), jnp.float32, jnp.log(0.8), jnp.log(1.25)))
    return baseline * roughness


def draw_bounds(key, part):
    lowest = jnp.array([1.8, 5.5], jnp.float32)
    highest = jnp.array([2.4, 6.5], jnp.float32)
    return jax.random.uniform(jax.random.fold_in(key, 13), (2,), jnp.float32, lowest, highest)


def place_ends(result, stream_key, smallest, largest):
    extent = result.shape
    index_at = [jax.random.randint(jax.random.fold_in(stream_key, axis), (), 0, extent[axis]) for axis in range(len(extent))]
    result = result.at[tuple(index_at)].set(smallest)
    longest = extent.index(max(extent))
    index_at[longest] = (index_at[longest] + 1) % extent[longest]
    return result.at[tuple(index_at)].set(largest)


def block_levels(own_key, shape, split, low, largest):
    gain = 1.0
    for position, shards_of in split:
        draws = jax.random.uniform(jax.random.fold_in(jax.random.fold_in(own_key, 6), position), (shards_of,), jnp.float32, low / len(split), largest / len(split))
        gain = gain * jnp.repeat(jnp.exp(draws), shape[position] // shards_of).reshape((-1,) + (1,) * (len(shape) - 1 - position))
    return gain


def scatter_about(stream_key, dims, deviation, bound, shards=(), kind=jnp.bfloat16):
    values = jax.random.normal(stream_key, dims, jnp.float32) * deviation
    if len(shards) > 0:
        values = block_levels(stream_key, dims, shards, -0.22, 0.18) * values
    return jnp.clip(values, min=-bound, max=bound).astype(kind)


def setup_inputs(seed: int = 0) -> dict:
    arg_keys = jax.random.split(jax.random.key(seed), 7)
    start = draw_start(jax.random.fold_in(arg_keys[6], 71), 0)
    couplings = scatter_about(arg_keys[1], (NODES // TILE, TILES_ROW, TILE, TILE), (TILES_ROW * TILE) ** -0.5, 0.15625, ((0, 32),))
    tile_cols = place_ends(jax.random.randint(arg_keys[2], (NODES // TILE, TILES_ROW), 0, 5 * ROWS_DEV // TILE), jax.random.fold_in(arg_keys[2], 1), 0, (5 * ROWS_DEV // TILE) - 1).astype(jnp.int32)
    stiffness = jnp.clip(jnp.exp(math.log(4.0) - 0.98082925 * jax.random.uniform(arg_keys[3], (NODES,), jnp.float32) ** block_levels(arg_keys[3], (NODES,), ((0, 32),), -0.2, 0.2)), 1.5, 4.0)
    masses = draw_masses(jax.random.fold_in(arg_keys[6], 71), 0)
    bounds = draw_bounds(jax.random.fold_in(arg_keys[6], 71), 0)
    return dict(start=start, couplings=couplings, tile_cols=tile_cols, stiffness=stiffness, masses=masses, bounds=bounds)


def coupling_products(vectors, couplings, tile_cols):
    tile_size = couplings.shape[-1]
    width = vectors.shape[1]
    per = ROWS_DEV // tile_size
    rounded = lax.optimization_barrier(vectors.astype(jnp.bfloat16)).astype(jnp.float32)
    grid = rounded.reshape(N_ROW, N_COL, ROWS_DEV, width)
    padded = jnp.pad(grid, ((1, 1), (1, 1), (0, 0), (0, 0)))
    tiles = couplings.reshape(N_ROW * N_COL, per, TILES_ROW, tile_size, tile_size)
    columns = tile_cols.reshape(N_ROW * N_COL, per, TILES_ROW)
    owners = jnp.arange(N_ROW * N_COL, dtype=jnp.int32)
    zero = jnp.zeros((), jnp.int32)

    def one_block(inputs):
        owner, block_tiles, block_cols = inputs
        block_row = (owner // N_COL).astype(jnp.int32)
        block_col = (owner % N_COL).astype(jnp.int32)
        window = lax.dynamic_slice(padded, (block_row, block_col, zero, zero), (3, 3, ROWS_DEV, width))
        stack = jnp.stack([window[1, 1], window[0, 1], window[2, 1], window[1, 0], window[1, 2]])
        stack = stack.reshape(5 * per, tile_size, width)
        picked = stack[block_cols]
        product = jnp.einsum('psab,psbk->pak', block_tiles.astype(jnp.float32), picked, precision=lax.Precision.HIGHEST)
        return product.reshape(ROWS_DEV, width)
    blocks = lax.map(one_block, (owners, tiles, columns))
    return blocks.reshape(NODES, width)

def matmul_high(left, right):
    return jnp.dot(left.astype(jnp.float32), right.astype(jnp.float32), precision=lax.Precision.HIGHEST, preferred_element_type=jnp.float32)

def cholesky_inverse(gram, identity):
    factor = jnp.linalg.cholesky(gram)
    return lax.linalg.triangular_solve(factor, identity, left_side=True, lower=True)

def reference(start, couplings, tile_cols, stiffness, masses, bounds):
    stiff_column = stiffness[:, None]
    inverse_mass = 1.0 / masses[:, None]

    def stiff(vectors):
        return stiff_column * vectors - coupling_products(vectors, couplings, tile_cols)
    cut_low = bounds[0]
    cut_high = bounds[1]
    center = 0.5 * (cut_high + cut_low)
    radius = 0.5 * (cut_high - cut_low)
    scale_first = -radius / center
    twice_inverse = 2.0 / scale_first
    previous = start
    current = scale_first / radius * (stiff(start) * inverse_mass - center * start)
    scale_now = scale_first
    for iteration in range(DEGREE - 1):
        scale_next = 1.0 / (twice_inverse - scale_now)
        following = 2.0 * scale_next / radius * (stiff(current) * inverse_mass - center * current) - scale_now * scale_next * previous
        previous, current, scale_now = (current, following, scale_next)
    weighted = masses[:, None] / NODES
    identity = jnp.eye(current.shape[1], dtype=jnp.float32)
    gram = matmul_high(current.T, weighted * current)
    projected = matmul_high(current.T, stiff(current) / NODES)
    inverse = cholesky_inverse(gram, identity)
    basis = matmul_high(current, inverse.T)
    ritz = matmul_high(matmul_high(inverse, projected), inverse.T)
    return (basis, ritz)
```

```python
import functools

import jax
import jax.numpy as jnp
from jax import lax
from jax.experimental import pallas as pl
from jax.experimental.pallas import tpu as pltpu
from jax.sharding import PartitionSpec as P

DEGREE = 8
SUB = 8
CHAINS = 2
VMEM = pl.BlockSpec(memory_space=pltpu.VMEM)
SMEM = pl.BlockSpec(memory_space=pltpu.SMEM)
ANY = pl.BlockSpec(memory_space=pl.ANY)
PARAMS = pltpu.CompilerParams(vmem_limit_bytes=16 << 20)
f32, bf16 = jnp.float32, jnp.bfloat16
shape_of = jax.ShapeDtypeStruct


def matmul_high(left, right, dims):
    return lax.dot_general(
        left,
        right,
        (dims, ((), ())),
        precision=lax.Precision.HIGHEST,
        preferred_element_type=f32,
    )


def pairing(count, first):
    pairs = []
    for i in range(first, count - 1, 2):
        pairs += [(i, i + 1), (i + 1, i)]
    if pairs and first:
        pairs += [(0, count - 1), (count - 1, 0)]
    return pairs


PAIRINGS = (("col", 0), ("row", 1), ("row", 0), ("col", 1))


def used_pairings():
    return [(a, f) for a, f in PAIRINGS if pairing(lax.axis_size(a), f)]


def exchange(rounded):
    received = [
        lax.ppermute(rounded, axis, pairing(lax.axis_size(axis), first))
        for axis, first in used_pairings()
    ]
    return [rounded] + received


def slot_table():
    places = {key: i + 1 for i, key in enumerate(used_pairings())}
    nowhere = len(places) + 1
    slots = [0]
    for axis in ("row", "col"):
        here, count = lax.axis_index(axis), lax.axis_size(axis)
        even, odd = places.get((axis, 0), nowhere), places.get((axis, 1), nowhere)
        is_even = here % 2 == 0
        slots += [
            jnp.where(here > 0, jnp.where(is_even, odd, even), nowhere),
            jnp.where(here < count - 1, jnp.where(is_even, even, odd), nowhere),
        ]
    return [jnp.asarray(s, jnp.int32) for s in slots], nowhere


def fill(stack, blocks, per_block):
    tile_size = stack.shape[2]
    for i, block in enumerate(blocks):
        for t in range(per_block):
            stack[i * per_block + t] = block[:, t * tile_size : (t + 1) * tile_size]
    stack[len(blocks) * per_block] = jnp.zeros(stack.shape[1:], stack.dtype)


def coupled(table, couplings, stack, p):
    total = None
    for s in range(couplings.shape[1]):
        part = lax.dot_general(
            stack[table[p, s]],
            couplings[p, s],
            (((1,), (1,)), ((), ())),
            preferred_element_type=f32,
        )
        total = part if total is None else total + part
    return total


def prepare_kernel(start, *outs):
    flipped = start[...].T
    rows = outs[0].shape[0]
    for c in range(len(outs) // 2):
        piece = flipped[c * rows : (c + 1) * rows, :]
        outs[2 * c][...] = piece
        outs[2 * c + 1][...] = piece.astype(bf16)


def load_kernel(source, target, sem):
    copy = pltpu.make_async_copy(source, target, sem)
    copy.start()
    copy.wait()


def step_kernel(halo, order, first, table, coef, couplings, *refs):
    blocks, refs = refs[:halo], refs[halo:]
    if first:
        now, a, b, out, rounded, stack = refs
        before = None
    else:
        now, before, a, b, out, rounded, stack = refs
    per_block, _, tile_size, _ = couplings.shape
    fill(stack, blocks, per_block)
    scale, center, keep = coef[0, order], coef[1, order], coef[2, order]
    for p in range(per_block):
        here = pl.ds(p * tile_size, tile_size)
        product = coupled(table, couplings, stack, p)
        vectors = now[:, here]
        following = scale * ((a[:, here] * vectors - product) * b[:, here] - center * vectors)
        if before is not None:
            following = following - keep * before[:, here]
        out[:, here] = following
        rounded[:, here] = following.astype(bf16)


def gram_kernel(chains, weights, *refs):
    parts, (out, full) = refs[:chains], refs[chains:]
    rows = parts[0].shape[0]
    for c in range(chains):
        full[pl.ds(c * rows, rows), :] = parts[c][...]
    vectors = full[...]
    out[...] = matmul_high(vectors, weights[...] * vectors, ((1,), (1,)))


def project_kernel(halo, chains, chain, nodes, table, couplings, *refs):
    blocks, parts = refs[:halo], refs[halo : halo + chains]
    a, out, stack, full, stiffed = refs[halo + chains :]
    per_block, _, tile_size, _ = couplings.shape
    fill(stack, blocks, per_block)
    rows = parts[0].shape[0]
    for c in range(chains):
        full[pl.ds(c * rows, rows), :] = parts[c][...]
    for p in range(per_block):
        here = pl.ds(p * tile_size, tile_size)
        product = coupled(table, couplings, stack, p)
        stiffed[:, here] = (a[:, here] * parts[chain][:, here] - product) / nodes
    out[...] = matmul_high(stiffed[...], full[...], ((1,), (1,)))


def final_kernel(chains, parity, mine, other, *refs):
    parts, (basis, ritz, full, work, inverse) = refs[:chains], refs[chains:]
    width = mine.shape[0]
    vec_rows = parts[0].shape[0]
    for c in range(chains):
        full[pl.ds(c * vec_rows, vec_rows), :] = parts[c][...]
    is_even = parity[0] == 0
    first, second = mine[...], other[...]
    rows = lax.broadcasted_iota(jnp.int32, (width, width), 0)
    lanes = lax.broadcasted_iota(jnp.int32, (width, width), 1)
    work[0] = jnp.where(is_even, first, second)
    work[1] = jnp.where(rows == lanes, 1.0, 0.0)
    sub = lax.broadcasted_iota(jnp.int32, (SUB, width), 0)

    def spread(value, i):
        return jnp.broadcast_to(value[i : i + 1, :], (SUB, width))

    def column(value, i):
        return jnp.broadcast_to(value[:, i : i + 1], (SUB, width))

    for k in range(width // SUB):
        here = pl.ds(k * SUB, SUB)
        left, right = work[0, here, :], work[1, here, :]
        cols = [column(left, k * SUB + i) for i in range(SUB)]
        lefts, rights, factors = [], [], []
        for i in range(SUB):
            pivot = spread(cols[i], i)
            root = lax.rsqrt(pivot)
            root = root * (1.5 - 0.5 * pivot * root * root)
            row_left, row_right = spread(left, i) * root, spread(right, i) * root
            row_cols = [spread(cols[m], i) * root if m > i else None for m in range(SUB)]
            lefts.append(row_left)
            rights.append(row_right)
            factors.append((root, row_cols))
            if i + 1 < SUB:
                scaled = jnp.where(sub > i, cols[i] * root, 0.0)
                left = left - scaled * row_left
                right = right - scaled * row_right
                for m in range(i + 1, SUB):
                    cols[m] = cols[m] - scaled * row_cols[m]
        done = rights[0]
        for i in range(1, SUB):
            done = jnp.where(sub == i, rights[i], done)
        inverse[here, :] = done
        for below in range(k + 1, width // SUB):
            there = pl.ds(below * SUB, SUB)
            left, right = work[0, there, :], work[1, there, :]
            cols = [column(left, k * SUB + i) for i in range(SUB)]
            for i in range(SUB):
                root, row_cols = factors[i]
                scaled = cols[i] * root
                left = left - scaled * lefts[i]
                right = right - scaled * rights[i]
                for m in range(i + 1, SUB):
                    cols[m] = cols[m] - scaled * row_cols[m]
            work[0, there, :] = left
            work[1, there, :] = right
    lower = inverse[...]
    basis[...] = matmul_high(full[...], lower, ((0,), (1,)))
    projected = jnp.where(is_even, second, first)
    half = matmul_high(lower, projected, ((1,), (1,)))
    ritz[...] = matmul_high(half, lower, ((1,), (1,)))


def call(kernel, outs, specs, args, scratch=(), flops=0, size=1 << 20, name=None):
    return pl.pallas_call(
        kernel,
        out_shape=outs,
        in_specs=specs + [VMEM] * (len(args) - len(specs)),
        out_specs=jax.tree.map(lambda _: VMEM, outs),
        scratch_shapes=list(scratch),
        compiler_params=PARAMS,
        cost_estimate=pl.CostEstimate(flops=flops, bytes_accessed=size, transcendentals=0),
        name=name,
    )(*args)


def per_device(start, couplings, tile_cols, stiffness, masses, bounds):
    rows_dev, width = start.shape
    per_block, stored, tile_size, _ = couplings.shape
    node_count = rows_dev * lax.axis_size("row") * lax.axis_size("col")
    rows = width // CHAINS
    wide, narrow = shape_of((rows, rows_dev), f32), shape_of((rows, rows_dev), bf16)
    flops = 2 * per_block * stored * tile_size * tile_size * rows

    prepared = call(prepare_kernel, (wide, narrow) * CHAINS, [], [start], flops=1 << 20, name="prepare")
    now, rounded = list(prepared[0::2]), list(prepared[1::2])
    before = [None] * CHAINS
    couplings = call(
        load_kernel,
        shape_of(couplings.shape, couplings.dtype),
        [ANY],
        [couplings],
        [pltpu.SemaphoreType.DMA],
        flops=1 << 28,
        name="load",
    )

    slots, nowhere = slot_table()
    block_of, tile_of = tile_cols // per_block, tile_cols % per_block
    slot = jnp.zeros_like(block_of)
    for q in range(1, 5):
        slot = jnp.where(block_of == q, slots[q], slot)
    table = slot * per_block + jnp.where(slot == nowhere, 0, tile_of)

    a, inverse_mass = stiffness[None, :], (1.0 / masses)[None, :]
    weights = (masses / node_count)[None, :]

    cut_low, cut_high = bounds[0], bounds[1]
    center = 0.5 * (cut_high + cut_low)
    radius = 0.5 * (cut_high - cut_low)
    scale = -radius / center
    twice_inverse = 2.0 / scale
    coefs = [(scale / radius, center, jnp.zeros((), f32))]
    for _ in range(DEGREE - 1):
        following = 1.0 / (twice_inverse - scale)
        coefs.append((2.0 * following / radius, center, scale * following))
        scale = following
    coef = jnp.stack([jnp.stack(list(c)) for c in zip(*coefs)])

    stack = pltpu.VMEM((nowhere * per_block + 1, rows, tile_size), bf16)

    for order in range(DEGREE):
        for c in range(CHAINS):
            blocks = exchange(rounded[c])
            old = [] if before[c] is None else [before[c]]
            args = [table, coef, couplings, *blocks, now[c], *old, a, inverse_mass]
            following, rounded[c] = call(
                functools.partial(step_kernel, len(blocks), order, not old),
                (wide, narrow),
                [SMEM, SMEM],
                args,
                [stack],
                flops=flops,
                name=f"step{order}",
            )
            before[c], now[c] = now[c], following

    full = pltpu.VMEM((width, rows_dev), f32)
    gram = call(
        functools.partial(gram_kernel, CHAINS),
        shape_of((width, width), f32),
        [],
        [weights, *now],
        [full],
        flops=flops,
        name="gram",
    )
    parts = []
    for c in range(CHAINS):
        blocks = exchange(rounded[c])
        parts.append(
            call(
                functools.partial(project_kernel, len(blocks), CHAINS, c, node_count),
                shape_of((rows, width), f32),
                [SMEM],
                [table, couplings, *blocks, *now, a],
                [stack, full, pltpu.VMEM((rows, rows_dev), f32)],
                flops=flops,
                name="project",
            )
        )
    projected = jnp.concatenate(parts, axis=0)

    parity = lax.axis_index("row") % 2
    swap = pairing(lax.axis_size("row"), 0)
    keep = jnp.where(parity == 0, gram, projected)
    send = jnp.where(parity == 0, projected, gram)
    mine = keep + lax.ppermute(send, "row", swap)
    for axis, bit in (("row", 2), ("col", 1)):
        count = lax.axis_size(axis)
        while bit < count:
            mine = mine + lax.ppermute(mine, axis, [(i, i ^ bit) for i in range(count)])
            bit *= 2
    other = lax.ppermute(mine, "row", swap)

    return call(
        functools.partial(final_kernel, CHAINS),
        (shape_of((rows_dev, width), f32), shape_of((width, width), f32)),
        [SMEM],
        [parity[None], mine, other, *now],
        [full, pltpu.VMEM((2, width, width), f32), pltpu.VMEM((width, width), f32)],
        flops=flops,
        name="final",
    )


def solution(mesh):
    for axis in ("row", "col"):
        count = mesh.shape[axis]
        if count & (count - 1) or count < 2:
            raise ValueError("axis size")
    return jax.shard_map(
        per_device,
        mesh=mesh,
        in_specs=(
            P(("row", "col"), None),
            P(("row", "col"), None, None, None),
            P(("row", "col"), None),
            P(("row", "col")),
            P(("row", "col")),
            P(),
        ),
        out_specs=(P(("row", "col"), None), P()),
        check_vma=False,
    )
```
